32 devices in a mesh: dp: 4 (over x, core), vocab: 8 (over z, y).
Axes of the slice: x: 2, y: 2, z: 4, core: 2. Of those that a mesh axis runs over, the one named last changes fastest.
Arguments:
- hidden: bfloat16 [512, 8192], P('dp'), may hold values from -600 to 600
- out_weight: bfloat16 [8192, 98304], P('dp', 'vocab'), may hold values from -0.5 to 0.5
- targets: int32 [512], P('dp'), may hold values from 0 to 98303
- segment: int32 [512], P('dp'), may hold values from 0 to 15, never falling along the last dimension, each value on 1 to 64 neighbouring positions
- loss_mask: int32 [512], P('dp'), may hold values 0 or 1
- outside_count: int32 [16], replicated, may hold values from 0 to 3
Outputs:
- token_loss: float32 [512], P('dp')
- sample_loss: float32 [16], replicated
The draws below stay inside these ranges and needn't reach their ends.
All inputs are finite; a program needn't handle non-finite values. No bound on the sum of `loss_mask` on one device may be relied on, other than what follows from the above.
Results may differ from the reference program's by a relative error of at most 0.0003.
Values may be sent and summed in bfloat16 or wider, within the bound.
No kernel may reach another device: no remote copies, remote signals or barrier semaphores. Data moves between devices by JAX's collectives and lax.ppermute only.
A program may use at most 128 MiB of HBM per device.

```python
import math
import jax
import jax.numpy as jnp
import numpy as np
from jax import lax

D = 8192
V = 98304
TOKENS = 512
SAMPLES = 16
SEG_MOST = 64


def weight_full(key):
    base = jax.random.normal(jax.random.fold_in(key, 7), (D, V), jnp.float32) * D ** (-0.5)
    return base


def draw_out_weight(key, part):
    return weight_full(key).astype(jnp.bfloat16)


def draw_hidden(key, part):
    states = jax.random.normal(jax.random.fold_in(key, 21), (TOKENS, D), jnp.float32) * 3.0
    return states.astype(jnp.bfloat16)


def set_ends(entries, key, smallest, top_value):
    index_at = [jax.random.randint(jax.random.fold_in(key, axis), (), 0, length) for axis, length in enumerate(entries.shape)]
    longest = entries.shape.index(max(entries.shape))
    neighbour = index_at[:longest] + [(index_at[longest] + 1) % entries.shape[longest]] + index_at[longest + 1:]
    return entries.at[tuple(index_at)].set(smallest).at[tuple(neighbour)].set(top_value)


def ranked_wide(stream_key, shape, number_of, slope):
    portions = [min(1 << octave, number_of + 1 - (1 << octave)) * (1 << 20) // math.isqrt((1 << octave) ** slope) + 1 for octave in range((number_of + 1).bit_length()) if 1 << octave <= number_of]
    spread = 1 + sum(portions) // (1 << 30)
    grid = np.cumsum(np.array([max(1, weight // spread) for weight in portions]))
    lot = jax.random.randint(jax.random.fold_in(stream_key, 1), shape, 0, int(grid[len(portions) - 1]))
    start = jnp.left_shift(1, jnp.searchsorted(jnp.asarray(grid, jnp.int32), lot, side="right").astype(jnp.int32))
    standing = start - 1 + jax.random.randint(jax.random.fold_in(stream_key, 4), shape, 0, 1 << 30) % jnp.minimum(start, number_of + 1 - start)
    return jax.random.permutation(jax.random.fold_in(stream_key, 2), number_of)[standing].astype(jnp.int32)


def length_profile(amount, total, reach, skew):
    weights = [(1 << 20) // math.isqrt(standing ** skew) + 1 for standing in range(2, amount + 1)]
    surplus, holding = total - reach - (amount - 1), [1] * (amount - 1)
    while surplus > 0:
        candidates = [i for i in range(amount - 1) if holding[i] < reach]
        pool, left = sum([weights[i] for i in candidates]), surplus
        for i in candidates:
            extra = min(reach - holding[i], max(1, left * weights[i] // pool), surplus)
            holding[i] = holding[i] + extra
            surplus = surplus - extra
    return np.array([reach] + holding)


def uneven(rng, number_of, total, reach, skew):
    if number_of == 2:
        one = jax.random.randint(rng, (), max(1, total - reach), min(reach, total - 1) + 1)
        return jnp.stack([one, total - one])
    lengths = jnp.asarray(length_profile(number_of, total, reach, skew), jnp.int32)
    couples = (number_of - 1) // 2
    donor, receiver = lengths[1:1 + 2 * couples:2], lengths[2:2 + 2 * couples:2]
    slack = jnp.minimum(donor - 1, reach - receiver)
    moved = jax.random.randint(jax.random.fold_in(rng, 1), (couples,), 0, 1 << 20) % (slack + 1)
    lengths = lengths.at[1:1 + 2 * couples:2].set(donor - moved).at[2:2 + 2 * couples:2].set(receiver + moved)
    return lengths[jax.random.permutation(jax.random.fold_in(rng, 2), number_of)]


def setup_inputs(seed: int = 0) -> dict:
    seeds = jax.random.split(jax.random.key(seed), 7)
    return {
        "hidden": draw_hidden(jax.random.fold_in(seeds[6], 71), 0),
        "out_weight": draw_out_weight(jax.random.fold_in(seeds[6], 71), 0),
        "targets": set_ends(ranked_wide(seeds[2], (TOKENS,), V, 2), jax.random.fold_in(seeds[2], 3), 0, V - 1).astype(jnp.int32),
        "segment": jnp.searchsorted(jnp.cumsum(uneven(seeds[3], SAMPLES, TOKENS, SEG_MOST, 2)), jnp.arange(TOKENS), side="right").astype(jnp.int32),
        "loss_mask": set_ends((jax.random.randint(seeds[4], (TOKENS,), 0, 4) < 3).astype(jnp.int32), jax.random.fold_in(seeds[4], 1), 0, 1),
        "outside_count": set_ends(jax.random.randint(seeds[5], (SAMPLES,), 0, 4), jax.random.fold_in(seeds[5], 1), 0, 3).astype(jnp.int32),
    }


def reference(hidden, out_weight, targets, segment, loss_mask, outside_count):
    block_rows = math.gcd(TOKENS, 256)
    block_count = TOKENS // block_rows
    hidden_blocks = hidden.reshape(block_count, block_rows, D)
    target_blocks = targets.reshape(block_count, block_rows)

    def one_block(pair):
        rows_block, target_block = pair
        logits = jnp.dot(rows_block, out_weight, preferred_element_type=jnp.float32)
        largest = jnp.max(logits, axis=1)
        lse = largest + jnp.log(jnp.sum(jnp.exp(logits - largest[:, None]), axis=1))
        picked = jnp.take_along_axis(logits, target_block[:, None].astype(jnp.int32), axis=1)[:, 0]
        return lse - picked

    token_loss = lax.map(one_block, (hidden_blocks, target_blocks)).reshape(TOKENS)
    onehot = (segment[:, None] == jnp.arange(SAMPLES, dtype=jnp.int32)[None, :]).astype(jnp.float32)
    weights = loss_mask.astype(jnp.float32)
    loss_sum = jnp.dot(token_loss * weights, onehot, precision=lax.Precision.HIGHEST)
    count = jnp.dot(weights, onehot, precision=lax.Precision.HIGHEST)
    denom = jnp.maximum(count + outside_count.astype(jnp.float32), 1.0)
    return token_loss, loss_sum / denom
```

```python
import functools
import jax
import jax.numpy as jnp
from jax import lax
from jax.experimental import pallas as pl
from jax.experimental.pallas import tpu as pltpu
from jax.sharding import PartitionSpec as P

CORES = 2
POWER = 7
LANES = 128
VMEM = 48 * 1024 * 1024


def encode(x, scale):
    x = x * scale
    square = x * x
    return (x * square * square * square).astype(jnp.bfloat16)


def decode(y, scale):
    y = y.astype(jnp.float32)
    size = jnp.exp2(jnp.log2(jnp.abs(y)) * (1.0 / POWER)) * (1.0 / scale)
    return jnp.where(y == 0.0, 0.0, jnp.where(y < 0.0, -size, size))


def dot(h_ref, w_ref):
    return jnp.dot(h_ref[...], w_ref[...], preferred_element_type=jnp.float32)


def partial_kernel(off_ref, h_ref, w_ref, out_ref):
    out_ref[...] = dot(h_ref, w_ref)


def send_kernel(scale, off_ref, h_ref, w_ref, sib_ref, out_ref):
    out_ref[...] = encode(dot(h_ref, w_ref) + sib_ref[...], scale)


def stats_kernel(scale, far, first, last, tile, *refs):
    off_ref, h_ref, w_ref, sib_ref = refs[:4]
    far_refs = refs[4:4 + far]
    target_ref = refs[4 + far]
    rest = refs[5 + far:]
    state, rest = (None, rest) if first else (rest[0], rest[1:])
    out_ref, m_ref, s_ref, t_ref = rest
    step = pl.program_id(0)

    @pl.when(step == 0)
    def _():
        if first:
            m_ref[...] = jnp.full_like(m_ref, -jnp.inf)
            s_ref[...] = jnp.zeros_like(s_ref)
            t_ref[...] = jnp.zeros_like(t_ref)
        else:
            m_ref[...] = state[0]
            s_ref[...] = state[1]
            t_ref[...] = state[2]

    logits = dot(h_ref, w_ref) + sib_ref[...]
    for ref in far_refs:
        logits = logits + decode(ref[...], scale)
    tokens = logits.shape[0]
    wanted = target_ref[...] - off_ref[1] - step * tile
    lane = lax.broadcasted_iota(jnp.int32, (tokens, LANES), 1)
    groups = [logits[:, k:k + LANES] for k in range(0, tile, LANES)]
    old = m_ref[...]
    new = functools.reduce(jnp.maximum, groups, old)
    total = s_ref[...] * jnp.exp(old - new)
    hit = t_ref[...]
    for k, group in enumerate(groups):
        total = total + jnp.exp(group - new)
        hit = hit + jnp.where(lane + k * LANES == wanted, group, 0.0)
    m_ref[...] = new
    s_ref[...] = total
    t_ref[...] = hit

    @pl.when(step == pl.num_programs(0) - 1)
    def _():
        if not last:
            out_ref[0] = new
            out_ref[1] = total
            out_ref[2] = hit
        else:
            top = jnp.max(new, axis=1, keepdims=True)
            total_1 = jnp.sum(total * jnp.exp(new - top), axis=1, keepdims=True)
            hit_1 = jnp.sum(hit, axis=1, keepdims=True)
            packed = jnp.where(lane == 0, top, jnp.where(lane == 1, total_1, hit_1))
            rows = jnp.transpose(packed)[:8]
            per = tokens // LANES
            tile_rows = [rows[q:q + 1, b * LANES:(b + 1) * LANES] for q in range(3) for b in range(per)]
            tile_rows.append(jnp.zeros((out_ref.shape[1] - 3 * per, LANES), jnp.float32))
            block = jnp.concatenate(tile_rows, axis=0)
            for d in range(out_ref.shape[0]):
                out_ref[d] = block


def loss_kernel(chips, vocab, samples, me_ref, stats_ref, meta_ref, outside_ref, loss_ref, sample_ref, all_ref):
    per = meta_ref.shape[0] // chips
    for holder in range(chips):
        base = holder * CORES * vocab
        block = stats_ref[base:base + CORES * vocab]
        m, s, t = (block[:, q * per:(q + 1) * per, :] for q in range(3))
        top = jnp.max(m, axis=0)
        total = jnp.sum(s * jnp.exp(m - top[None]), axis=0)
        owner = (holder - 1) % chips
        all_ref[owner * per:(owner + 1) * per, :] = top + jnp.log(total) - jnp.sum(t, axis=0)
    ids = lax.broadcasted_iota(jnp.int32, (samples, LANES), 0)
    loss_sum = jnp.zeros((samples, LANES), jnp.float32)
    count = jnp.zeros((samples, LANES), jnp.float32)
    for d in range(chips * per):
        same = meta_ref[d, 1:2, :] == ids
        weight = meta_ref[d, 2:3, :].astype(jnp.float32)
        loss_sum = loss_sum + jnp.where(same, weight * all_ref[d:d + 1, :], 0.0)
        count = count + jnp.where(same, weight, 0.0)
    loss_sum = jnp.sum(loss_sum, axis=1, keepdims=True)
    count = jnp.sum(count, axis=1, keepdims=True)
    denom = jnp.maximum(count + outside_ref[...].astype(jnp.float32), 1.0)
    sample_ref[...] = loss_sum / denom
    loss_ref[...] = all_ref[pl.ds(me_ref[0], 1), :]


def chunks_of(tiles):
    sizes, left = [], tiles
    for share in (1, 2, 3, 3, 2):
        take = max(1, share * tiles // 12)
        if left - take >= 1:
            sizes.append(take)
            left -= take
    sizes.append(left)
    return sizes


def body(devices, chips, vocab, hidden, out_weight, targets, segment, loss_mask, outside_count):
    block, depth = hidden.shape[0], out_weight.shape[0]
    half = out_weight.shape[1] // CORES
    tokens = CORES * block
    samples = outside_count.shape[0]
    tile = next(t for t in (512, 256, 128) if half % t == 0)
    tiles = half // tile
    bound = 600.0 * 0.5 * depth * CORES
    scale = 2.0 ** -8
    while (bound * scale * 2) ** POWER < 2.0 ** 124:
        scale *= 2.0
    while (bound * scale) ** POWER > 2.0 ** 124:
        scale *= 0.5
    me = lax.axis_index("dp")
    vm = lax.axis_index("vocab")
    core, chip = me % CORES, me // CORES
    dp = chips * CORES
    swap = [(d, d ^ 1) for d in range(dp)]

    def hop(shift, flip=0):
        return [(d, (d // CORES + shift) % chips * CORES + (d % CORES ^ flip)) for d in range(dp)]

    group = 4
    while vocab % group or block % (16 * group):
        group //= 2
    part = block // group
    mine = vm % group
    strip = lax.dynamic_slice_in_dim(hidden, mine * part, part, 0)

    def columns(a, index):
        return lax.dynamic_slice_in_dim(a, index * depth, depth, 1)

    sibling = lax.ppermute(columns(hidden, me ^ 1), "dp", swap)
    meta = jnp.concatenate(
        [targets[None], segment[None], loss_mask[None], jnp.zeros((5, block), jnp.int32)], axis=0)
    fetched = {}
    for shift in range(1, chips):
        dest = (chip + shift) % chips * CORES
        near = lax.ppermute(columns(strip, dest + core), "dp", hop(shift))
        cross = lax.ppermute(columns(strip, dest + 1 - core), "dp", hop(shift, 1))
        fetched[shift] = (near, cross)
    own = jnp.zeros((CORES, block, depth), hidden.dtype)
    own = lax.dynamic_update_slice(own, columns(hidden, me)[None], (core, 0, 0))
    own = lax.dynamic_update_slice(own, sibling[None], (1 - core, 0, 0))
    own = own.reshape(tokens, depth)
    metas = jnp.zeros((dp,) + meta.shape, jnp.int32)
    metas = lax.dynamic_update_slice(metas, meta[None], (me, 0, 0))
    for shift in range(chips):
        for flip in range(CORES):
            if shift or flip:
                got = lax.ppermute(meta, "dp", hop(shift, flip))
                source = (chip - shift) % chips * CORES + (core ^ flip)
                metas = lax.dynamic_update_slice(metas, got[None], (source, 0, 0))

    def gathered(shift):
        near, cross = fetched[shift]
        pair = jnp.zeros((CORES, 1, part, depth), hidden.dtype)
        pair = lax.dynamic_update_slice(pair, near[None, None], (core, 0, 0, 0))
        pair = lax.dynamic_update_slice(pair, cross[None, None], (1 - core, 0, 0, 0))
        whole = jnp.zeros((CORES, group, part, depth), hidden.dtype)
        for k in range(group):
            got = pair if k == 0 else lax.ppermute(pair, "vocab", [(i, i ^ k) for i in range(vocab)])
            whole = lax.dynamic_update_slice(whole, got, (0, mine ^ k, 0, 0))
        return whole.reshape(tokens, depth)

    starts = (jnp.stack([(1 - core) * tiles, 0 * core]), jnp.stack([core * tiles, vm * CORES * half + core * half]))

    def call(kernel, rows, which, start, size, operands, specs, out_shape, out_spec, scratch=(), name=None):
        offsets = starts[which] + jnp.array([start, start * tile], jnp.int32)
        return pl.pallas_call(
            kernel,
            grid_spec=pltpu.PrefetchScalarGridSpec(
                num_scalar_prefetch=1,
                grid=(size,),
                in_specs=[
                    pl.BlockSpec((tokens, depth), lambda i, off: (0, 0)),
                    pl.BlockSpec((depth, tile), lambda i, off: (0, off[0] + i)),
                ] + list(specs),
                out_specs=out_spec,
                scratch_shapes=list(scratch),
            ),
            out_shape=out_shape,
            cost_estimate=pl.CostEstimate(
                flops=2 * tokens * depth * tile * size,
                bytes_accessed=2 * depth * tile * size,
                transcendentals=0,
            ),
            compiler_params=pltpu.CompilerParams(
                dimension_semantics=("arbitrary",), vmem_limit_bytes=VMEM),
            name=name,
        )(offsets, rows, out_weight, *operands)

    def tiled(start):
        return pl.BlockSpec((tokens, tile), lambda i, off: (0, start + i))

    def partial(rows, start, size, name):
        return call(partial_kernel, rows, 0, start, size, (), (),
                    jax.ShapeDtypeStruct((tokens, size * tile), jnp.float32), tiled(0), name=name)

    sizes = chunks_of(tiles)
    begins = [sum(sizes[:j]) for j in range(len(sizes))]
    pieces = [(begins[j], sizes[j]) for j in range(min(2, len(sizes)))]
    done = sum(size for _, size in pieces)
    if done < tiles:
        pieces.append((done, tiles - done))

    sent = [[] for _ in sizes]
    for shift in range(1, chips):
        rows = own if shift == 1 else gathered(chips - shift + 1)
        swapped = [lax.ppermute(partial(rows, b, n, f"near_{shift}_{b}"), "dp", swap) for b, n in pieces]
        for j, (b, n) in enumerate(zip(begins, sizes)):
            where = max(p for p in range(len(pieces)) if pieces[p][0] <= b)
            out = call(functools.partial(send_kernel, scale), rows, 1, b, n,
                       (swapped[where],), (tiled(b - pieces[where][0]),),
                       jax.ShapeDtypeStruct((tokens, n * tile), jnp.bfloat16), tiled(0), name=f"send_{shift}_{b}")
            sent[j].append(lax.ppermute(out, "dp", hop(shift)))

    rows = gathered(1)
    swapped = lax.ppermute(partial(rows, 0, tiles, "kept"), "dp", swap)
    before = (chip - 1) % chips
    wanted = lax.dynamic_slice_in_dim(metas[:, 0, :], before * CORES, CORES, 0).reshape(tokens, 1)
    state = None
    for j, (b, n) in enumerate(zip(begins, sizes)):
        first, last = j == 0, j == len(sizes) - 1
        operands = [swapped] + sent[j] + [wanted] + ([] if first else [state])
        specs = [tiled(b)] + [tiled(0)] * len(sent[j]) + [pl.BlockSpec((tokens, 1), lambda i, off: (0, 0))]
        if not first:
            specs.append(pl.BlockSpec((3, tokens, LANES), lambda i, off: (0, 0, 0)))
        shape = (devices, 8, LANES) if last else (3, tokens, LANES)
        state = call(
            functools.partial(stats_kernel, scale, len(sent[j]), first, last, tile), rows, 1, b, n,
            operands, specs, jax.ShapeDtypeStruct(shape, jnp.float32),
            pl.BlockSpec(shape, lambda i, off: (0, 0, 0)),
            [pltpu.VMEM((tokens, LANES), jnp.float32)] * 3, name=f"stats_{b}")
    everyone = lax.all_to_all(state, ("dp", "vocab"), 0, 0, tiled=True)
    loss, sample = pl.pallas_call(
        functools.partial(loss_kernel, chips, vocab, samples),
        in_specs=[pl.BlockSpec(memory_space=pltpu.SMEM)] + [pl.BlockSpec(memory_space=pltpu.VMEM)] * 3,
        out_specs=[pl.BlockSpec(memory_space=pltpu.VMEM)] * 2,
        out_shape=[jax.ShapeDtypeStruct((1, block), jnp.float32), jax.ShapeDtypeStruct((samples, 1), jnp.float32)],
        scratch_shapes=[pltpu.VMEM((dp, LANES), jnp.float32)],
        name="loss",
    )(me[None], everyone, metas, outside_count[:, None])
    return loss.reshape(block), sample.reshape(samples)


def solution(mesh):
    dp, vocab = mesh.shape["dp"], mesh.shape["vocab"]
    return jax.shard_map(
        functools.partial(body, dp * vocab, dp // CORES, vocab),
        mesh=mesh,
        in_specs=(P("dp", None), P("dp", "vocab"), P("dp"), P("dp"), P("dp"), P()),
        out_specs=(P("dp"), P()),
        check_vma=False,
    )
```
